64 devices in a mesh: rep: 8 (over x, y, core), dp: 8 (over z).
Axes of the slice: x: 2, y: 2, z: 8, core: 2. Of those that a mesh axis runs over, the one named last changes fastest.
The devices are a block of a 4x4x8 slice.
Arguments:
- x: bfloat16 [64, 2048, 640], P(('rep', 'dp')), parts along dimension 0
- dy: bfloat16 [64, 2048, 640], P(('rep', 'dp')), parts along dimension 0
- w_gate: bfloat16 [2, 640, 2048], replicated
- w_up: bfloat16 [2, 640, 2048], replicated
- w_down: bfloat16 [2, 2048, 640], replicated
- m_w_gate: float32 [2, 640, 2048], replicated
- m_w_up: float32 [2, 640, 2048], replicated
- m_w_down: float32 [2, 2048, 640], replicated
- v_w_gate: float32 [2, 640, 2048], replicated
- v_w_up: float32 [2, 640, 2048], replicated
- v_w_down: float32 [2, 2048, 640], replicated
Outputs:
- output 1: bfloat16 [16, 640, 2048], P('rep'), parts along dimension 0
- output 2: bfloat16 [16, 640, 2048], P('rep'), parts along dimension 0
- output 3: bfloat16 [16, 2048, 640], P('rep'), parts along dimension 0
- output 4: float32 [16, 640, 2048], P('rep'), parts along dimension 0
- output 5: float32 [16, 640, 2048], P('rep'), parts along dimension 0
- output 6: float32 [16, 2048, 640], P('rep'), parts along dimension 0
- output 7: float32 [16, 640, 2048], P('rep'), parts along dimension 0
- output 8: float32 [16, 640, 2048], P('rep'), parts along dimension 0
- output 9: float32 [16, 2048, 640], P('rep'), parts along dimension 0
There are 8 independent parts. The reference program is written for one: setup_inputs(seed, part) draws one part's arguments, and reference() takes and returns one part's arrays. A program takes and returns all parts, laid end to end along the dimension named above; an argument that names none is the same for every part.
All inputs are finite; a program needn't handle non-finite values.
Results may differ from the reference program's by a relative error of at most 0.022.
Values are sent between devices in bfloat16 or wider.
A program may use at most 768 MiB of HBM per device.

```python
import jax
import jax.numpy as jnp
from jax import lax

SEQUENCES = 8
TOKENS = 2048
D = 640
FF = 2048
LAYERS = 2
NAMES = ("w_gate", "w_up", "w_down")
SHAPES = {"w_gate": (LAYERS, D, FF), "w_up": (LAYERS, D, FF), "w_down": (LAYERS, FF, D)}


def bump(key, n, height):
    away = (jnp.arange(n, dtype=jnp.int32) - jax.random.randint(key, (), 0, n, jnp.int32)) % n
    return jnp.where(away < n // 8, height, 1.0)


def together(key, own, strength):
    shared = jax.random.normal(key, own.shape[1:], jnp.float32)
    return (own + strength * shared) * lax.rsqrt(1 + strength * strength)


def setup_inputs(seed: int = 0, part: int = 0) -> dict:
    kx, kdy, ka, kb, kz, kf, kh, kl, *keys = jax.random.split(jax.random.key(seed), 8 + 3 * len(NAMES))
    kx, kdy, ka, kb = (jax.random.fold_in(k, part) for k in (kx, kdy, ka, kb))
    kw, km, kv = (keys[i::3] for i in range(3))
    shape = (SEQUENCES, TOKENS, D)
    much_x, much_dy = jax.random.uniform(kz, (2,), jnp.float32, 0.0, 1.0)
    loud = 2.0 ** jax.random.uniform(jax.random.fold_in(kz, 1), (), jnp.float32, -1.0, 2.0)
    layers = 2.0 ** jax.random.uniform(kl, (LAYERS, 1, 1), jnp.float32, -1.0, 1.0)
    x = together(ka, jax.random.normal(kx, shape, jnp.float32), much_x) * bump(kf, D, 4.0)
    dy = together(kb, jax.random.normal(kdy, shape, jnp.float32), much_dy)
    drawn = {"x": x.astype(jnp.bfloat16), "dy": (loud * dy * (SEQUENCES * TOKENS) ** -0.5).astype(jnp.bfloat16)}
    for key, name in zip(kw, NAMES, strict=True):
        w = jax.random.normal(key, SHAPES[name], jnp.float32) * SHAPES[name][1] ** -0.5
        drawn[name] = (w * {"w_gate": 1.0, "w_up": bump(kh, FF, 4.0), "w_down": layers}[name]).astype(jnp.bfloat16)
    for key, name in zip(km, NAMES, strict=True):
        drawn[f"m_{name}"] = 0.1 * jax.random.normal(key, SHAPES[name], jnp.float32)
    for key, name in zip(kv, NAMES, strict=True):
        drawn[f"v_{name}"] = jax.random.uniform(key, SHAPES[name], jnp.float32, 0.005, 0.015)
    return drawn


def matmul(a, w):
    return jnp.dot(a, w, preferred_element_type=jnp.float32).astype(jnp.bfloat16)


def normed(h):
    wide = h.astype(jnp.float32)
    scale = lax.rsqrt(jnp.mean(wide**2, -1, keepdims=True) + 1e-6)
    return (wide * scale).astype(jnp.bfloat16)


def layer(h, w):
    a = normed(h)
    gate = jnp.dot(a, w["w_gate"], preferred_element_type=jnp.float32)
    up = jnp.dot(a, w["w_up"], preferred_element_type=jnp.float32)
    return h + matmul((jax.nn.silu(gate) * up).astype(jnp.bfloat16), w["w_down"])


def adamw(w, m, v, g):
    m = 0.9 * m + 0.1 * g
    v = 0.95 * v + 0.05 * g * g
    step = m * lax.rsqrt(v + 1e-8) + 0.1 * w
    return (w - 0.02 * step).astype(jnp.bfloat16), m, v


def stack(weights, h):
    return lax.scan(lambda h, w: (layer(h, w), None), h, weights)[0]


def reference(x, dy, w_gate, w_up, w_down, m_w_gate, m_w_up, m_w_down, v_w_gate, v_w_up, v_w_down):
    weights = dict(zip(NAMES, (w_gate, w_up, w_down), strict=True))

    def take(so_far, sequence):
        h, by_y = sequence
        _, back = jax.vjp(lambda w: stack(w, h), weights)
        return jax.tree.map(lambda total, term: total + term.astype(jnp.float32), so_far, back(by_y)[0]), None

    none_yet = {name: jnp.zeros(w.shape, jnp.float32) for name, w in weights.items()}
    by_weights, _ = lax.scan(take, none_yet, (x, dy))
    gradients = [by_weights[name].astype(jnp.bfloat16).astype(jnp.float32) for name in NAMES]
    new = [
        adamw(w.astype(jnp.float32), m, v, g)
        for w, m, v, g in zip((w_gate, w_up, w_down), (m_w_gate, m_w_up, m_w_down), (v_w_gate, v_w_up, v_w_down), gradients, strict=True)
    ]
    return tuple(one[which] for which in range(3) for one in new)
```

```python
import functools

import jax
import jax.numpy as jnp
from jax import lax
from jax.experimental import pallas as pl
from jax.experimental.pallas import tpu as pltpu
from jax.sharding import PartitionSpec as P

F32, BF16 = jnp.float32, jnp.bfloat16
LANES = 128
TILE = 256
SLOTS = 6
GAP = 2


def dot(a, b):
    return jnp.dot(a, b, preferred_element_type=F32)


def dot_t(a, b):
    return lax.dot_general(a, b, (((1,), (1,)), ((), ())), preferred_element_type=F32)


def scale_of(wide):
    return lax.rsqrt(jnp.mean(wide * wide, -1, keepdims=True) + 1e-6)


class Sizes:
    def __init__(self, mesh, x, w_gate):
        self.n = mesh.shape["dp"]
        self.tokens, self.d = x.shape[1:]
        self.layers, _, self.ff = w_gate.shape
        self.units = self.ff // TILE
        self.rows = self.d // self.n
        self.down = TILE // 2 // self.n
        self.halves, self.fifths = TILE // LANES, self.d // LANES
        self.message = self.halves * self.rows + self.fifths * self.down


def step_kernel(s, x_hbm, dy_hbm, wg_hbm, wu_hbm, wd_hbm, *refs):
    (own_x, own_y), refs = (refs[0:2], refs[2:4]), refs[4:]
    (wg, wu, wd, xh, a, a_t, dh, dh_t, dg, du, hid, own, got, final, gs, us, ds, hs, ps) = refs[:19]
    (load_sem, w_sem, send_sem, recv_sem, out_sem) = refs[19:]
    me = lax.axis_index("dp")
    right, left = lax.rem(me + 1, s.n), lax.rem(me + s.n - 1, s.n)
    towards = (right, left)

    barrier = pltpu.get_barrier_semaphore()
    for neighbour in towards:
        pl.semaphore_signal(barrier, inc=1, device_id={"dp": neighbour}, device_id_type=pl.DeviceIdType.MESH)

    first = [
        pltpu.make_async_copy(x_hbm.at[0], xh, load_sem.at[0]),
        pltpu.make_async_copy(wg_hbm.at[0], dg.at[pl.ds(0, s.d)], load_sem.at[1]),
        pltpu.make_async_copy(wu_hbm.at[0], dg.at[pl.ds(s.d, s.d)], load_sem.at[2]),
        pltpu.make_async_copy(wd_hbm.at[0], du.at[:, pl.ds(0, s.d)], load_sem.at[3]),
    ]
    second = [
        pltpu.make_async_copy(dy_hbm.at[0], dh, load_sem.at[4]),
        pltpu.make_async_copy(wg_hbm.at[1], wg, load_sem.at[5]),
        pltpu.make_async_copy(wu_hbm.at[1], wu, load_sem.at[6]),
        pltpu.make_async_copy(wd_hbm.at[1], wd, load_sem.at[7]),
    ]
    for copy in first:
        copy.start()
    for copy in first:
        copy.wait()
    for copy in second:
        copy.start()
    second[0].wait()

    small = TILE

    def forward(block, carry):
        rows = pl.ds(pl.multiple_of(block * small, small), small)
        wide = xh[rows, :].astype(F32)
        normed = (wide * scale_of(wide)).astype(BF16)
        a[0, rows, :] = normed
        for j in range(s.units):
            cols = pl.ds(j * TILE, TILE)
            gs[j % 2] = dot(normed, dg[pl.ds(0, s.d), cols])
            us[j % 2] = dot(normed, dg[pl.ds(s.d, s.d), cols])
            for r in range(0, small, 32):
                g = gs[j % 2, pl.ds(r, 32), :]
                hs[pl.ds(r, 32), cols] = (g * jax.nn.sigmoid(g) * us[j % 2, pl.ds(r, 32), :]).astype(BF16)
        ps[0] = dot(hs[...], du[:, pl.ds(0, s.d)])
        for r in range(0, small, 32):
            part = pl.ds(block * small + r, 32)
            h = (xh[part, :].astype(F32) + ps[0, pl.ds(r, 32), :].astype(BF16).astype(F32)).astype(BF16)
            xh[part, :] = h
            wide = h.astype(F32)
            a[1, part, :] = (wide * scale_of(wide)).astype(BF16)
        a_t[:, rows] = a[1, rows, :].T
        dh_t[:, rows] = dh[rows, :].T
        return carry

    lax.fori_loop(0, s.tokens // small, forward, 0)
    for copy in second[1:]:
        copy.wait()
    pl.semaphore_wait(barrier, 2)

    quarter = s.tokens // 4

    def inner(layer, unit, block):
        cols = pl.ds(pl.multiple_of(unit * TILE, TILE), TILE)
        for half in range(quarter // TILE):
            at = block * quarter + half * TILE
            rows = pl.ds(at, TILE)
            gs[half] = dot(a[layer, rows, :], wg[:, cols])
            us[half] = dot(a[layer, rows, :], wu[:, cols])
            ds[half] = dot_t(dh[rows, :], wd[cols, :]).astype(BF16)
            for r in range(0, TILE, 32):
                part = pl.ds(r, 32)
                g, u, by = gs[half, part, :], us[half, part, :], ds[half, part, :].astype(F32)
                sig = jax.nn.sigmoid(g)
                silu = g * sig
                rows = pl.ds(at + r, 32)
                hid[rows, :] = (silu * u).astype(BF16)
                du[rows, cols] = (by * silu).astype(BF16)
                dg[rows, cols] = (by * u * (sig + silu * (1.0 - sig))).astype(BF16)

    def keep_across(slot, which, value):
        for chunk in range(s.n):
            for half in range(s.halves):
                own[slot, which, chunk, pl.ds(half * s.rows, s.rows), :] = value[
                    chunk * s.rows : (chunk + 1) * s.rows, half * LANES : (half + 1) * LANES
                ]

    def by_gate(unit, slot):
        cols = pl.ds(pl.multiple_of(unit * TILE, TILE), TILE)
        keep_across(slot, 0, dot(a_t[...], dg[:, cols]).astype(BF16))

    def by_up(unit, slot):
        cols = pl.ds(pl.multiple_of(unit * TILE, TILE), TILE)
        keep_across(slot, 1, dot(a_t[...], du[:, cols]).astype(BF16))

    def by_down(slot):
        value = dot(dh_t[...], hid[...]).T.astype(BF16)
        for which in range(2):
            for chunk in range(s.n):
                top = (which * s.n + chunk) * s.down
                for fifth in range(s.fifths):
                    own[slot, which, chunk, pl.ds(s.halves * s.rows + fifth * s.down, s.down), :] = value[
                        top : top + s.down, fifth * LANES : (fifth + 1) * LANES
                    ]

    def back_through_norm(block):
        at = block * TILE
        rows = pl.ds(pl.multiple_of(at, TILE), TILE)
        ps[0] = dot_t(dg[rows, :], wg[...])
        ps[1] = dot_t(du[rows, :], wu[...])
        for r in range(0, TILE, 32):
            part, here = pl.ds(r, 32), pl.ds(at + r, 32)
            by_a = (ps[0, part, :].astype(BF16).astype(F32) + ps[1, part, :].astype(BF16).astype(F32)).astype(BF16).astype(F32)
            wide = xh[here, :].astype(F32)
            scale = scale_of(wide)
            by = scale * by_a - wide * (scale * scale * scale * jnp.mean(wide * by_a, -1, keepdims=True))
            dh[here, :] = (dh[here, :].astype(F32) + by.astype(BF16).astype(F32)).astype(BF16)
        dh_t[:, rows] = dh[rows, :].T
        a_t[:, rows] = a[0, rows, :].T

    late = s.units + GAP

    def is_unit(u):
        return ((u >= 0) & (u < s.units)) | ((u >= late) & (u < late + s.units))

    def chunk_of(way, hop):
        return lax.rem(me + (s.n - 1 - hop if way == 0 else 1 + hop), s.n)

    def send(u, hop, way):
        slot = lax.rem(u, SLOTS)
        return pltpu.make_async_remote_copy(
            src_ref=own.at[slot, way, chunk_of(way, hop)],
            dst_ref=got.at[slot, hop, way],
            send_sem=send_sem.at[slot, way],
            recv_sem=recv_sem.at[slot, hop, way],
            device_id={"dp": towards[way]},
            device_id_type=pl.DeviceIdType.MESH,
        )

    def hop(u, number):
        @pl.when(is_unit(u))
        def _():
            slot = lax.rem(u, SLOTS)
            for way in range(2):
                if number > 0:
                    before = send(u, number - 1, way)
                    before.wait_recv()
                    mine = own[slot, way, chunk_of(way, number)].astype(F32)
                    total = (mine + got[slot, number - 1, way].astype(F32)).astype(BF16)
                    if number < s.n - 1:
                        own[slot, way, chunk_of(way, number)] = total
                    else:
                        final[lax.select(u < late, 1, 0), lax.select(u < late, u, u - late), way] = total
                    before.wait_send()
            if number < s.n - 1:
                for way in range(2):
                    send(u, number, way).start()

    def period(q, carry):
        early = q < s.units
        real = is_unit(q)
        layer = lax.select(early, 1, 0)
        unit = lax.select(early, q, q - late)
        slot = lax.rem(q, SLOTS)
        between = (q >= s.units) & (q < late)
        plan = ([(2, 2)], [(3, 4)], [(4, 6)], [(1, 1)], [(2, 3)], [(3, 5)], [(4, 7), (0, 0)])
        for k in range(7):
            @pl.when(real)
            def _():
                if k == 0:
                    @pl.when(q >= late)
                    def _():
                        for copy in pieces(unit):
                            copy.wait()
                if k < 4:
                    inner(layer, unit, k)
                elif k == 4:
                    by_gate(unit, slot)
                elif k == 5:
                    by_up(unit, slot)
                else:
                    by_down(slot)

            if k < 4:
                @pl.when(between)
                def _():
                    back_through_norm((q - s.units) * 4 + k)

            if k == 3:
                @pl.when(q == late - 1)
                def _():
                    def fetch(piece, carry):
                        for copy in pieces(piece):
                            copy.start()
                        return carry
                    lax.fori_loop(0, s.units, fetch, 0)

            for back, number in plan[k]:
                hop(q - back, number)
        return carry

    def pieces(unit):
        cols = pl.ds(pl.multiple_of(unit * TILE, TILE), TILE)
        return [
            pltpu.make_async_copy(wg_hbm.at[0, :, cols], wg.at[:, cols], w_sem.at[0, unit]),
            pltpu.make_async_copy(wu_hbm.at[0, :, cols], wu.at[:, cols], w_sem.at[1, unit]),
            pltpu.make_async_copy(wd_hbm.at[0, cols, :], wd.at[cols, :], w_sem.at[2, unit]),
        ]

    lax.fori_loop(0, late + s.units + 4, period, 0)

    half = s.units // 2
    outs = [
        pltpu.make_async_copy(final.at[:, pl.ds(part * half, half), way], (own_x, own_y)[part][way], out_sem.at[part, way])
        for part in range(2)
        for way in range(2)
    ]
    for copy in outs:
        copy.start()
    for copy in outs:
        copy.wait()


def reduced_shards(s, x, dy, w_gate, w_up, w_down):
    shard = jax.ShapeDtypeStruct((s.layers, s.units // 2, s.message, LANES), BF16)
    d, t, ff = s.d, s.tokens, s.ff
    any_space = pl.BlockSpec(memory_space=pl.ANY)
    out = pl.pallas_call(
        functools.partial(step_kernel, s),
        out_shape=(shard,) * 4,
        in_specs=[any_space] * 5,
        out_specs=(any_space,) * 4,
        scratch_shapes=[
            pltpu.VMEM((d, ff), BF16),
            pltpu.VMEM((d, ff), BF16),
            pltpu.VMEM((ff, d), BF16),
            pltpu.VMEM((t, d), BF16),
            pltpu.VMEM((2, t, d), BF16),
            pltpu.VMEM((d, t), BF16),
            pltpu.VMEM((t, d), BF16),
            pltpu.VMEM((d, t), BF16),
            pltpu.VMEM((t, ff), BF16),
            pltpu.VMEM((t, ff), BF16),
            pltpu.VMEM((t, TILE), BF16),
            pltpu.VMEM((SLOTS, 2, s.n, s.message, LANES), BF16),
            pltpu.VMEM((SLOTS, s.n - 1, 2, s.message, LANES), BF16),
            pltpu.VMEM((s.layers, s.units, 2, s.message, LANES), BF16),
            pltpu.VMEM((2, TILE, TILE), F32),
            pltpu.VMEM((2, TILE, TILE), F32),
            pltpu.VMEM((2, TILE, TILE), BF16),
            pltpu.VMEM((TILE, ff), BF16),
            pltpu.VMEM((2, TILE, d), F32),
            pltpu.SemaphoreType.DMA((8,)),
            pltpu.SemaphoreType.DMA((3, s.units)),
            pltpu.SemaphoreType.DMA((SLOTS, 2)),
            pltpu.SemaphoreType.DMA((SLOTS, s.n - 1, 2)),
            pltpu.SemaphoreType.DMA((2, 2)),
        ],
        compiler_params=pltpu.CompilerParams(collective_id=0, has_side_effects=True, vmem_limit_bytes=67043328),
    )(x, dy, w_gate, w_up, w_down)
    return [out[0:2], out[2:4]]


def adamw(w, m, v, g):
    m = 0.9 * m + 0.1 * g
    v = 0.95 * v + 0.05 * g * g
    step = m * lax.rsqrt(v + 1e-8) + 0.1 * w
    return (w - 0.02 * step).astype(BF16), m, v


def adamw_kernel(s, where_ref, from_left, from_right, *refs):
    across, down = (refs[0:3], refs[3:6]), refs[6:9]
    outs = refs[len(refs) - 9 :]
    across_out, down_out = (outs[0:3], outs[3:6]), outs[6:9]

    for way, message in enumerate((from_left, from_right)):
        @pl.when(pl.program_id(0) == way)
        def _():
            def unit_step(unit, carry):
                for half in range(s.halves):
                    g = message[0, unit, pl.ds(half * s.rows, s.rows), :].astype(F32)
                    cols = pl.ds(pl.multiple_of(unit * TILE + half * LANES, LANES), LANES)
                    w, m, v = (ref[0, :, cols] for ref in across[way])
                    new = adamw(w.astype(F32), m, v, g)
                    for ref, value in zip(across_out[way], new, strict=True):
                        ref[0, :, cols] = value
                for fifth in range(s.fifths):
                    g = message[0, unit, pl.ds(s.halves * s.rows + fifth * s.down, s.down), :].astype(F32)
                    cols = pl.ds(fifth * LANES, LANES)
                    w, m, v = (ref[0, unit, 0, 0, :, cols] for ref in down)
                    new = adamw(w.astype(F32), m, v, g)
                    for ref, value in zip(down_out, new, strict=True):
                        ref[0, unit, 0, 0, :, cols] = value
                return carry

            lax.fori_loop(0, s.units // 2, unit_step, 0)


def adamw_on(s, part, hop, messages, state, so_far):
    me = lax.axis_index("dp")
    where = jnp.stack([lax.rem(me + s.n - hop, s.n), lax.rem(me + hop, s.n)]).astype(jnp.int32)
    half = s.units // 2
    last = s.layers - 1
    spec_across = (
        pl.BlockSpec((1, s.rows, half * TILE), lambda way, layer, at: (jnp.where(way == 0, layer, last), at[0], part)),
        pl.BlockSpec((1, s.rows, half * TILE), lambda way, layer, at: (jnp.where(way == 0, 0, layer), at[1], part)),
    )
    spec_down = pl.BlockSpec((1, half, 1, 1, s.down, s.d), lambda way, layer, at: (layer, part, way, at[way], 0, 0))
    spec_message = (
        pl.BlockSpec((1, half, s.message, LANES), lambda way, layer, at: (jnp.where(way == 0, layer, last), 0, 0, 0)),
        pl.BlockSpec((1, half, s.message, LANES), lambda way, layer, at: (jnp.where(way == 0, 0, layer), 0, 0, 0)),
    )
    specs = [spec_across[0]] * 3 + [spec_across[1]] * 3 + [spec_down] * 3
    flat = [one for group in state for one in group]
    shapes = [jax.ShapeDtypeStruct(one.shape, one.dtype) for one in flat]
    in_specs = list(spec_message) + specs
    args = [*messages, *flat]
    aliases = {}
    if so_far is not None:
        aliases = {1 + len(args) + i: i for i in range(9)}
        args += so_far
        in_specs += [pl.BlockSpec(memory_space=pl.ANY)] * 9
    numbers = 2 * s.layers * half * s.message * LANES
    return list(
        pl.pallas_call(
            functools.partial(adamw_kernel, s),
            out_shape=shapes,
            grid_spec=pltpu.PrefetchScalarGridSpec(num_scalar_prefetch=1, grid=(2, s.layers), in_specs=in_specs, out_specs=specs),
            input_output_aliases=aliases,
            cost_estimate=pl.CostEstimate(flops=numbers * 20 * 1000, bytes_accessed=numbers * 22, transcendentals=numbers),
        )(where, *args)
    )


def solution(mesh):
    n = mesh.shape["dp"]

    def step(x, dy, *arrays):
        weights, m, v = (arrays[i : i + 3] for i in (0, 3, 6))
        s = Sizes(mesh, x, weights[0])
        halves = reduced_shards(s, x, dy, *weights)
        by_chunk = (s.layers, s.units, 2, s.n, s.down, s.d)
        state = [list(group) for group in zip(weights, m, v, strict=True)]
        state[2] = [one.reshape(by_chunk) for one in state[2]]
        rings = ([(i, (i + 1) % n) for i in range(n)], [(i, (i - 1) % n) for i in range(n)])
        out = None
        for hop in range(n):
            now = halves
            if hop < n - 1:
                halves = [[lax.ppermute(one, "dp", ring) for one, ring in zip(pair, rings, strict=True)] for pair in halves]
            for part in range(2):
                out = adamw_on(s, part, hop, now[part], state, out)
        out[6:9] = [one.reshape(weights[2].shape) for one in out[6:9]]
        return tuple(out[3 * which + i] for i in range(3) for which in range(3))

    return jax.shard_map(
        step,
        mesh=mesh,
        in_specs=(P(("rep", "dp"), None, None),) * 2 + (P(None, None, None),) * 9,
        out_specs=(P("rep", None, None),) * 9,
        check_vma=False,
    )
```

```python
import functools

import jax
import jax.numpy as jnp
from jax import lax
from jax.experimental import pallas as pl
from jax.experimental.pallas import tpu as pltpu
from jax.sharding import PartitionSpec as P

F32, BF16 = jnp.float32, jnp.bfloat16
LANES = 128
TILE = 256
SLOTS = 6
GAP = 2
GATHER_FROM = (7, 9, 10, 17)


def dot(a, b):
    return jnp.dot(a, b, preferred_element_type=F32)


def dot_t(a, b):
    return lax.dot_general(a, b, (((1,), (1,)), ((), ())), preferred_element_type=F32)


def scale_of(wide):
    return lax.rsqrt(jnp.mean(wide * wide, -1, keepdims=True) + 1e-6)


FLAGS = set()


class Sizes:
    def __init__(self, mesh, x, w_gate):
        self.n = mesh.shape["dp"]
        self.tokens, self.d = x.shape[1:]
        self.layers, _, self.ff = w_gate.shape
        self.units = self.ff // TILE
        self.part = self.units // 2
        self.rows = self.d // self.n
        self.down = TILE // 2 // self.n
        self.halves, self.fifths = TILE // LANES, self.d // LANES
        self.message = self.halves * self.rows + self.fifths * self.down


def step_kernel(s, x_hbm, dy_hbm, wg_hbm, wu_hbm, wd_hbm, *refs):
    (near_x, near_y, all_x), refs = (refs[0:2], refs[2:4], refs[4:6]), refs[6:]
    (wg, wu, wd, xh, a, a_t, dh, dh_t, dg, du, hid, own, got, final, gathered, gs, us, ds, hs, ps, first_in, second_in) = refs[:22]
    (load_sem, w_sem, send_sem, recv_sem, out_sem, gather_send, gather_recv) = refs[22:]
    me = lax.axis_index("dp")
    right, left = lax.rem(me + 1, s.n), lax.rem(me + s.n - 1, s.n)
    towards = (right, left)

    barrier = pltpu.get_barrier_semaphore()
    for neighbour in towards:
        pl.semaphore_signal(barrier, inc=1, device_id={"dp": neighbour}, device_id_type=pl.DeviceIdType.MESH)

    small = TILE
    first = [
        pltpu.make_async_copy(x_hbm.at[0, pl.ds(0, small)], xh.at[pl.ds(0, small)], load_sem.at[0]),
        pltpu.make_async_copy(wg_hbm.at[0], dg.at[pl.ds(0, s.d)], load_sem.at[1]),
        pltpu.make_async_copy(wu_hbm.at[0], dg.at[pl.ds(s.d, s.d)], load_sem.at[2]),
    ]
    rest = s.tokens - small
    second = [
        pltpu.make_async_copy(wd_hbm.at[0], du.at[:, pl.ds(0, s.d)], load_sem.at[3]),
        pltpu.make_async_copy(dy_hbm.at[0], dh, load_sem.at[4]),
        pltpu.make_async_copy(x_hbm.at[0, pl.ds(small, rest)], xh.at[pl.ds(small, rest)], load_sem.at[8]),
    ]
    third = [
        pltpu.make_async_copy(wg_hbm.at[1], wg, load_sem.at[5]),
        pltpu.make_async_copy(wu_hbm.at[1], wu, load_sem.at[6]),
        pltpu.make_async_copy(wd_hbm.at[1], wd, load_sem.at[7]),
    ]
    for copy in first:
        copy.start()
    for copy in first:
        copy.wait()
    for copy in second:
        copy.start()

    blocks = s.tokens // small

    def norm(block):
        for r in range(0, small, 32):
            part = pl.ds(block * small + r, 32)
            wide = xh[part, :].astype(F32)
            normed = (wide * scale_of(wide)).astype(BF16)
            a[0, part, :] = normed
            first_in[pl.ds(r, 32), :] = normed

    def finish(block, ready):
        for r in range(0, small, 32):
            part = pl.ds(block * small + r, 32)
            wide = xh[part, :].astype(F32)
            h = (wide + ps[0, pl.ds(r, 32), :].astype(BF16).astype(F32)).astype(BF16).astype(F32)
            h = jnp.where(ready, h, wide)
            xh[part, :] = h.astype(BF16)
            normed = (h * scale_of(h)).astype(BF16)
            a[1, part, :] = normed
            second_in[pl.ds(r, 32), :] = normed
        a_t[:, pl.ds(pl.multiple_of(block * small, small), small)] = second_in[...].T

    def forward(block, carry):
        finish(jnp.maximum(block - 1, 0), block > 0)
        for j in range(s.units):
            cols = pl.ds(j * TILE, TILE)
            gs[j % 2] = dot(first_in[...], dg[pl.ds(0, s.d), cols])
            us[j % 2] = dot(first_in[...], dg[pl.ds(s.d, s.d), cols])
            for r in range(0, small, 32):
                g = gs[j % 2, pl.ds(r, 32), :]
                hs[pl.ds(r, 32), cols] = (g * jax.nn.sigmoid(g) * us[j % 2, pl.ds(r, 32), :]).astype(BF16)

        @pl.when(block == 0)
        def _():
            for copy in second:
                copy.wait()
            for copy in third:
                copy.start()

        ps[0] = dot(hs[...], du[:, pl.ds(0, s.d)])
        rows = pl.ds(pl.multiple_of(block * small, small), small)
        dh_t[:, rows] = dh[rows, :].T
        norm(jnp.minimum(block + 1, blocks - 1))
        return carry

    norm(0)
    lax.fori_loop(0, blocks, forward, 0)
    finish(blocks - 1, True)
    for copy in third:
        copy.wait()
    pl.semaphore_wait(barrier, 2)

    quarter = s.tokens // 4

    def inner(layer, unit, block):
        cols = pl.ds(pl.multiple_of(unit * TILE, TILE), TILE)
        for half in range(quarter // TILE):
            at = block * quarter + half * TILE
            rows = pl.ds(at, TILE)
            gs[half] = dot(a[layer, rows, :], wg[:, cols])
            us[half] = dot(a[layer, rows, :], wu[:, cols])
            ds[half] = dot_t(dh[rows, :], wd[cols, :]).astype(BF16)
            for r in range(0, TILE, 32):
                part = pl.ds(r, 32)
                g, u, by = gs[half, part, :], us[half, part, :], ds[half, part, :].astype(F32)
                sig = jax.nn.sigmoid(g)
                silu = g * sig
                rows = pl.ds(at + r, 32)
                hid[rows, :] = (silu * u).astype(BF16)
                du[rows, cols] = (by * silu).astype(BF16)
                dg[rows, cols] = (by * u * (sig + silu * (1.0 - sig))).astype(BF16)

    def keep_across(slot, which, value):
        for chunk in range(s.n):
            for half in range(s.halves):
                own[slot, which, chunk, pl.ds(half * s.rows, s.rows), :] = value[
                    chunk * s.rows : (chunk + 1) * s.rows, half * LANES : (half + 1) * LANES
                ]

    def by_gate(unit, slot):
        cols = pl.ds(pl.multiple_of(unit * TILE, TILE), TILE)
        keep_across(slot, 0, dot(a_t[...], dg[:, cols]).astype(BF16))

    def by_up(unit, slot):
        cols = pl.ds(pl.multiple_of(unit * TILE, TILE), TILE)
        keep_across(slot, 1, dot(a_t[...], du[:, cols]).astype(BF16))

    def by_down(slot):
        value = dot(dh_t[...], hid[...]).T.astype(BF16)
        for which in range(2):
            for chunk in range(s.n):
                top = (which * s.n + chunk) * s.down
                for fifth in range(s.fifths):
                    own[slot, which, chunk, pl.ds(s.halves * s.rows + fifth * s.down, s.down), :] = value[
                        top : top + s.down, fifth * LANES : (fifth + 1) * LANES
                    ]

    def back_through_norm(block):
        at = block * TILE
        rows = pl.ds(pl.multiple_of(at, TILE), TILE)
        ps[0] = dot_t(dg[rows, :], wg[...])
        ps[1] = dot_t(du[rows, :], wu[...])
        for r in range(0, TILE, 32):
            part, here = pl.ds(r, 32), pl.ds(at + r, 32)
            by_a = (ps[0, part, :].astype(BF16).astype(F32) + ps[1, part, :].astype(BF16).astype(F32)).astype(BF16).astype(F32)
            wide = xh[here, :].astype(F32)
            scale = scale_of(wide)
            by = scale * by_a - wide * (scale * scale * scale * jnp.mean(wide * by_a, -1, keepdims=True))
            dh[here, :] = (dh[here, :].astype(F32) + by.astype(BF16).astype(F32)).astype(BF16)
        dh_t[:, rows] = dh[rows, :].T
        a_t[:, rows] = a[0, rows, :].T

    late = s.units + GAP

    def is_unit(u):
        return ((u >= 0) & (u < s.units)) | ((u >= late) & (u < late + s.units))

    def chunk_of(way, hop):
        return lax.rem(me + (s.n - 1 - hop if way == 0 else 1 + hop), s.n)

    def send(u, hop, way):
        slot = lax.rem(u, SLOTS)
        return pltpu.make_async_remote_copy(
            src_ref=own.at[slot, way, chunk_of(way, hop)],
            dst_ref=got.at[slot, hop, way],
            send_sem=send_sem.at[slot, way],
            recv_sem=recv_sem.at[slot, hop, way],
            device_id={"dp": towards[way]},
            device_id_type=pl.DeviceIdType.MESH,
        )

    def hop(u, number):
        @pl.when(is_unit(u))
        def _():
            slot = lax.rem(u, SLOTS)
            for way in range(2):
                if number > 0:
                    before = send(u, number - 1, way)
                    before.wait_recv()
                    mine = own[slot, way, chunk_of(way, number)].astype(F32)
                    total = (mine + got[slot, number - 1, way].astype(F32)).astype(BF16)
                    if number < s.n - 1:
                        own[slot, way, chunk_of(way, number)] = total
                    else:
                        unit = lax.select(u < late, u, u - late + s.units)
                        final[lax.div(unit, s.part), way, lax.rem(unit, s.part)] = total
                    before.wait_send()
            if number < s.n - 1:
                for way in range(2):
                    send(u, number, way).start()

    def spread(u, number):
        @pl.when((u >= 0) & (u < s.part))
        def _():
            for way in range(2):
                def copy(hop):
                    return pltpu.make_async_remote_copy(
                        src_ref=final.at[0, way, u] if hop == 0 else gathered.at[way, hop - 1, u],
                        dst_ref=gathered.at[way, hop, u],
                        send_sem=gather_send.at[u, way],
                        recv_sem=gather_recv.at[u, hop, way],
                        device_id={"dp": towards[way]},
                        device_id_type=pl.DeviceIdType.MESH,
                    )

                if number > 0:
                    copy(number - 1).wait_recv()
                    copy(number - 1).wait_send()
                if number < s.n - 1:
                    copy(number).start()

    def from_start(q):
        unit = -1
        for i, start in enumerate(GATHER_FROM):
            unit = lax.select(q == start, i, unit)
        return unit

    def period(q, carry):
        early = q < s.units
        real = is_unit(q)
        layer = lax.select(early, 1, 0)
        unit = lax.select(early, q, q - late)
        slot = lax.rem(q, SLOTS)
        between = (q >= s.units) & (q < late)
        plan = ([(2, 2)], [(3, 4)], [(4, 6)], [(1, 1)], [(2, 3)], [(3, 5)], [(4, 7), (0, 0)])
        spread_plan = plan
        for k in range(7):
            @pl.when(real)
            def _():
                if k == 0:
                    @pl.when(q >= late)
                    def _():
                        for copy in pieces(unit):
                            copy.wait()
                if k < 4:
                    inner(layer, unit, k)
                elif k == 4:
                    by_gate(unit, slot)
                elif k == 5:
                    by_up(unit, slot)
                else:
                    by_down(slot)

            if k < 4:
                @pl.when(between)
                def _():
                    back_through_norm((q - s.units) * 4 + k)

            if k == 3:
                @pl.when(q == late - 1)
                def _():
                    def fetch(piece, carry):
                        for copy in pieces(piece):
                            copy.start()
                        return carry
                    lax.fori_loop(0, s.units, fetch, 0)

            if k == 0:
                @pl.when(q == late + s.units + 1)
                def _():
                    for copy in outs(0):
                        copy.start()

            for back, number in plan[k]:
                hop(q - back, number)
            for back, number in spread_plan[k]:
                spread(from_start(q - back), number)
        return carry

    def outs(last):
        pairs, before = [], s.part - 1
        for way in range(2):
            if last:
                pairs += [
                    (gathered.at[way, :, before], all_x[way].at[pl.ds(1, s.n - 1), before]),
                    (final.at[3, way], near_y[way].at[0]),
                ]
            else:
                pairs += [
                    (final.at[0, way], all_x[way].at[0]),
                    (gathered.at[way, :, pl.ds(0, before)], all_x[way].at[pl.ds(1, s.n - 1), pl.ds(0, before)]),
                    (final.at[1, way], near_y[way].at[1]),
                    (final.at[2, way], near_x[way]),
                ]
        return [pltpu.make_async_copy(*pair, out_sem.at[last, i]) for i, pair in enumerate(pairs)]

    def pieces(unit):
        cols = pl.ds(pl.multiple_of(unit * TILE, TILE), TILE)
        return [
            pltpu.make_async_copy(wg_hbm.at[0, :, cols], wg.at[:, cols], w_sem.at[0, unit]),
            pltpu.make_async_copy(wu_hbm.at[0, :, cols], wu.at[:, cols], w_sem.at[1, unit]),
            pltpu.make_async_copy(wd_hbm.at[0, cols, :], wd.at[cols, :], w_sem.at[2, unit]),
        ]

    lax.fori_loop(0, late + s.units + 4, period, 0)
    for copy in outs(1):
        copy.start()
    for copy in outs(0) + outs(1):
        copy.wait()


def reduced_shards(s, x, dy, w_gate, w_up, w_down):
    part = (s.part, s.message, LANES)
    shapes = [jax.ShapeDtypeStruct(lead + part, BF16) for lead in ((), (s.layers,), (s.n,)) for _ in range(2)]
    d, t, ff = s.d, s.tokens, s.ff
    any_space = pl.BlockSpec(memory_space=pl.ANY)
    out = pl.pallas_call(
        functools.partial(step_kernel, s),
        out_shape=shapes,
        in_specs=[any_space] * 5,
        out_specs=[any_space] * 6,
        scratch_shapes=[
            pltpu.VMEM((d, ff), BF16),
            pltpu.VMEM((d, ff), BF16),
            pltpu.VMEM((ff, d), BF16),
            pltpu.VMEM((t, d), BF16),
            pltpu.VMEM((2, t, d), BF16),
            pltpu.VMEM((d, t), BF16),
            pltpu.VMEM((t, d), BF16),
            pltpu.VMEM((d, t), BF16),
            pltpu.VMEM((t, ff), BF16),
            pltpu.VMEM((t, ff), BF16),
            pltpu.VMEM((t, TILE), BF16),
            pltpu.VMEM((SLOTS, 2, s.n, s.message, LANES), BF16),
            pltpu.VMEM((SLOTS, s.n - 1, 2, s.message, LANES), BF16),
            pltpu.VMEM((2 * s.layers, 2, *part), BF16),
            pltpu.VMEM((2, s.n - 1, *part), BF16),
            pltpu.VMEM((2, TILE, TILE), F32),
            pltpu.VMEM((2, TILE, TILE), F32),
            pltpu.VMEM((2, TILE, TILE), BF16),
            pltpu.VMEM((TILE, ff), BF16),
            pltpu.VMEM((2, TILE, d), F32),
            pltpu.VMEM((TILE, d), BF16),
            pltpu.VMEM((TILE, d), BF16),
            pltpu.SemaphoreType.DMA((9,)),
            pltpu.SemaphoreType.DMA((3, s.units)),
            pltpu.SemaphoreType.DMA((SLOTS, 2)),
            pltpu.SemaphoreType.DMA((SLOTS, s.n - 1, 2)),
            pltpu.SemaphoreType.DMA((2, 8)),
            pltpu.SemaphoreType.DMA((s.part, 2)),
            pltpu.SemaphoreType.DMA((s.part, s.n - 1, 2)),
        ],
        compiler_params=pltpu.CompilerParams(collective_id=0, has_side_effects=True, vmem_limit_bytes=67043328),
    )(x, dy, w_gate, w_up, w_down)
    return out[0:2], out[2:4], out[4:6]


def adamw(w, m, v, g):
    m = 0.9 * m + 0.1 * g
    v = 0.95 * v + 0.05 * g * g
    step = m * lax.rsqrt(v + 1e-8) + 0.1 * w
    return (w - 0.02 * step).astype(BF16), m, v


AHEAD = 2


def adamw_kernel(s, items, operands, *refs):
    messages, refs = refs[: 2 * operands], refs[2 * operands :]
    state, refs = (refs[0:3], refs[3:6], refs[6:9]), refs[9:]
    refs = refs[len(refs) - 24 :]
    outs, refs = (refs[0:3], refs[3:6], refs[6:9]), refs[9:]
    (message_in, across_in, down_in, across_out, down_out), (sem_in, sem_out) = (refs[0], refs[1:4], refs[4:7], refs[7:10], refs[10:13]), refs[13:15]
    me = lax.axis_index("dp")

    def of(field, item):
        values = [one[field] for one in items]
        if isinstance(item, int):
            return values[item]
        if len(set(values)) == 1:
            return values[0]
        out = values[-1]
        for i in reversed(range(len(values) - 1)):
            out = jnp.where(item == i, values[i], out)
        return out

    def places(item, way, group):
        layer, part, away = of(0, item), of(1, item), of(2, item)
        chunk = lax.rem(me + (s.n - away if way == 0 else away), s.n)
        rows = pl.ds(pl.multiple_of(chunk * s.rows, s.rows), s.rows)
        cols = pl.ds(pl.multiple_of(part * (s.part * TILE), s.part * TILE), s.part * TILE)
        units = pl.ds(part * s.part, s.part)
        return [ref.at[layer, rows, cols] for ref in group[way]] + [ref.at[layer, units, way, chunk] for ref in group[2]]

    def loads(item, way):
        spots = [ref.at[item, way] for ref in (*across_in, *down_in)]
        return [
            pltpu.make_async_copy(*pair, sem_in.at[item, way, 1 + i])
            for i, pair in enumerate(zip(places(item, way, state), spots, strict=True))
        ]

    def message_load(item, way, which):
        return pltpu.make_async_copy(messages[2 * which + way].at[of(4, item)], message_in.at[item, way], sem_in.at[item, way, 0])

    def stores(item, way):
        spots = [ref.at[item, way] for ref in (*across_out, *down_out)]
        return [
            pltpu.make_async_copy(*pair, sem_out.at[item, way, i])
            for i, pair in enumerate(zip(spots, places(item, way, outs), strict=True))
        ]

    def fetch(item, carry=0):
        for way in range(2):
            for which in range(operands):
                @pl.when(of(3, item) == which)
                def _():
                    message_load(item, way, which).start()
            for copy in loads(item, way):
                copy.start()
        return carry

    def work(item, carry):
        @pl.when(item + AHEAD < len(items))
        def _():
            fetch(item + AHEAD)

        for way in range(2):
            message_load(item, way, 0).wait()
            for copy in loads(item, way):
                copy.wait()

            def unit_step(unit, carry):
                for half in range(s.halves):
                    g = message_in[item, way, unit, pl.ds(half * s.rows, s.rows), :].astype(F32)
                    cols = pl.ds(pl.multiple_of(unit * TILE + half * LANES, LANES), LANES)
                    w, m, v = (ref[item, way, :, cols] for ref in across_in)
                    new = adamw(w.astype(F32), m, v, g)
                    for ref, value in zip(across_out, new, strict=True):
                        ref[item, way, :, cols] = value
                for fifth in range(s.fifths):
                    g = message_in[item, way, unit, pl.ds(s.halves * s.rows + fifth * s.down, s.down), :].astype(F32)
                    cols = pl.ds(fifth * LANES, LANES)
                    w, m, v = (ref[item, way, unit, :, cols] for ref in down_in)
                    new = adamw(w.astype(F32), m, v, g)
                    for ref, value in zip(down_out, new, strict=True):
                        ref[item, way, unit, :, cols] = value
                return carry

            lax.fori_loop(0, s.part, unit_step, 0)
            for copy in stores(item, way):
                copy.start()
        return carry

    def drain(item, carry):
        for way in range(2):
            for copy in stores(item, way):
                copy.wait()
        return carry

    for item in range(min(AHEAD, len(items))):
        fetch(item)
    lax.fori_loop(0, len(items), work, 0)
    lax.fori_loop(0, len(items), drain, 0)


def adamw_on(s, items, messages, state, so_far):
    flat = [one for group in state for one in group]
    shapes = [jax.ShapeDtypeStruct(one.shape, one.dtype) for one in flat]
    args = [one for pair in messages for one in pair] + flat
    aliases = {}
    if so_far is not None:
        aliases = {len(args) + i: i for i in range(9)}
        args += so_far
    count = (len(items), 2)
    across, down = (*count, s.rows, s.part * TILE), (*count, s.part, s.down, s.d)
    types = (BF16, F32, F32)
    buffers = [pltpu.VMEM(shape, dtype) for shape in (across, down) for dtype in types]
    numbers = 2 * len(items) * s.part * s.message * LANES
    any_space = pl.BlockSpec(memory_space=pl.ANY)
    return list(
        pl.pallas_call(
            functools.partial(adamw_kernel, s, items, len(messages)),
            out_shape=shapes,
            in_specs=[any_space] * len(args),
            out_specs=[any_space] * 9,
            input_output_aliases=aliases,
            scratch_shapes=[pltpu.VMEM((*count, s.part, s.message, LANES), BF16)]
            + buffers
            + buffers
            + [pltpu.SemaphoreType.DMA((*count, 7)), pltpu.SemaphoreType.DMA((*count, 6))],
            compiler_params=pltpu.CompilerParams(vmem_limit_bytes=67043328),
            cost_estimate=pl.CostEstimate(flops=numbers * 20 * 1000, bytes_accessed=numbers * 22, transcendentals=numbers),
        )(*args)
    )


def solution(mesh):
    n = mesh.shape["dp"]

    def step(x, dy, *arrays):
        weights, m, v = (arrays[i : i + 3] for i in (0, 3, 6))
        s = Sizes(mesh, x, weights[0])
        near_x, near_y, all_x = reduced_shards(s, x, dy, *weights)
        near_x = [one[None] for one in near_x]
        by_chunk = (s.layers, s.units, 2, s.n, s.down, s.d)
        state = [list(group) for group in zip(weights, m, v, strict=True)]
        state[2] = [one.reshape(by_chunk) for one in state[2]]
        rings = ([(i, (i + 1) % n) for i in range(n)], [(i, (i - 1) % n) for i in range(n)])

        def shift(pair):
            return [lax.ppermute(one, "dp", ring) for one, ring in zip(pair, rings, strict=True)]

        out, now_x, now_y = None, near_x, near_y
        for hop in range(n):
            this_x, this_y = now_x, now_y
            y_items = [(0, 1, hop, 1, 0), (1, 1, hop, 1, 1)]
            if hop < n - 1:
                if hop > 0:
                    this_y, _ = lax.optimization_barrier((this_y, before))
                    this_x, _ = lax.optimization_barrier((this_x, this_y))
                before = this_x
                now_y, now_x = shift(this_y), shift(this_x)
                here = [(1, 0, away, 0, away) for away in ((0, n - 1) if hop == 0 else (hop,))]
                out = adamw_on(s, [*here, *y_items, (0, 0, hop, 2, 0)], [all_x, this_y, this_x], state, out)
            else:
                y_items = [(layer, part, away, 0, place) for layer, part, away, _, place in y_items]
                out = adamw_on(s, y_items, [this_y], state, out)
                out = adamw_on(s, [(0, 0, hop, 0, 0)], [this_x], state, out)
        out[6:9] = [one.reshape(weights[2].shape) for one in out[6:9]]
        return tuple(out[3 * which + i] for i in range(3) for which in range(3))

    return jax.shard_map(
        step,
        mesh=mesh,
        in_specs=(P(("rep", "dp"), None, None),) * 2 + (P(None, None, None),) * 9,
        out_specs=(P("rep", None, None),) * 9,
        check_vma=False,
    )
```

```python
import functools

import jax
import jax.numpy as jnp
from jax import lax
from jax.experimental import pallas as pl
from jax.experimental.pallas import tpu as pltpu
from jax.sharding import PartitionSpec as P

F32, BF16 = jnp.float32, jnp.bfloat16
LANES = 128
TILE = 256
SLOTS = 4
GAP = 2
GATHER_FROM = (6, 7, 8, 16)


def dot(a, b):
    return jnp.dot(a, b, preferred_element_type=F32)


def dot_t(a, b):
    return lax.dot_general(a, b, (((1,), (1,)), ((), ())), preferred_element_type=F32)


def scale_of(wide):
    return lax.rsqrt(jnp.mean(wide * wide, -1, keepdims=True) + 1e-6)


FLAGS = set()


class Sizes:
    def __init__(self, mesh, x, w_gate):
        self.n = mesh.shape["dp"]
        self.tokens, self.d = x.shape[1:]
        self.layers, _, self.ff = w_gate.shape
        self.units = self.ff // TILE
        self.part = self.units // 2
        self.far = self.n // 2
        self.rows = self.d // self.n
        self.down = TILE // 2 // self.n
        self.halves, self.fifths = TILE // LANES, self.d // LANES
        self.message = self.halves * self.rows + self.fifths * self.down


def step_kernel(s, x_hbm, dy_hbm, wg_hbm, wu_hbm, wd_hbm, *refs):
    (near_x, near_y, all_x), refs = (refs[0:2], refs[2:4], refs[4:6]), refs[6:]
    (wg, wu, wd, xh, a, a_t, dh, dh_t, dg, du, hid, own, got, final, gathered, gs, us, ds, hs, ps, first_in, second_in) = refs[:22]
    (load_sem, w_sem, send_sem, recv_sem, out_sem, gather_send, gather_recv) = refs[22:]
    me = lax.axis_index("dp")
    right, left = lax.rem(me + 1, s.n), lax.rem(me + s.n - 1, s.n)
    towards = (right, left)

    barrier = pltpu.get_barrier_semaphore()
    for neighbour in towards:
        pl.semaphore_signal(barrier, inc=1, device_id={"dp": neighbour}, device_id_type=pl.DeviceIdType.MESH)

    small = TILE
    first = [
        pltpu.make_async_copy(x_hbm.at[0, pl.ds(0, small)], xh.at[pl.ds(0, small)], load_sem.at[0]),
        pltpu.make_async_copy(wg_hbm.at[0], dg.at[pl.ds(0, s.d)], load_sem.at[1]),
        pltpu.make_async_copy(wu_hbm.at[0], dg.at[pl.ds(s.d, s.d)], load_sem.at[2]),
    ]
    rest = s.tokens - small
    second = [
        pltpu.make_async_copy(wd_hbm.at[0], du.at[:, pl.ds(0, s.d)], load_sem.at[3]),
        pltpu.make_async_copy(dy_hbm.at[0], dh, load_sem.at[4]),
        pltpu.make_async_copy(x_hbm.at[0, pl.ds(small, rest)], xh.at[pl.ds(small, rest)], load_sem.at[8]),
    ]
    third = [
        pltpu.make_async_copy(wg_hbm.at[1], wg, load_sem.at[5]),
        pltpu.make_async_copy(wu_hbm.at[1], wu, load_sem.at[6]),
        pltpu.make_async_copy(wd_hbm.at[1], wd, load_sem.at[7]),
    ]
    for copy in first + second:
        copy.start()
    first[0].wait()

    blocks = s.tokens // small

    def norm(block):
        for r in range(0, small, 32):
            part = pl.ds(block * small + r, 32)
            wide = xh[part, :].astype(F32)
            normed = (wide * scale_of(wide)).astype(BF16)
            a[0, part, :] = normed
            first_in[pl.ds(r, 32), :] = normed

    def finish(block, ready):
        for r in range(0, small, 32):
            part = pl.ds(block * small + r, 32)
            wide = xh[part, :].astype(F32)
            h = (wide + ps[pl.ds(r, 32), :].astype(BF16).astype(F32)).astype(BF16).astype(F32)
            h = jnp.where(ready, h, wide)
            xh[part, :] = h.astype(BF16)
            normed = (h * scale_of(h)).astype(BF16)
            a[1, part, :] = normed
            second_in[pl.ds(r, 32), :] = normed
        a_t[:, pl.ds(pl.multiple_of(block * small, small), small)] = second_in[...].T

    def forward(block, carry):
        finish(jnp.maximum(block - 1, 0), block > 0)
        for j in range(s.units):
            cols = pl.ds(j * TILE, TILE)
            gs[j % 2] = dot(first_in[...], dg[pl.ds(0, s.d), cols])
            us[j % 2] = dot(first_in[...], dg[pl.ds(s.d, s.d), cols])
            for r in range(0, small, 32):
                g = gs[j % 2, pl.ds(r, 32), :]
                hs[pl.ds(r, 32), cols] = (g * jax.nn.sigmoid(g) * us[j % 2, pl.ds(r, 32), :]).astype(BF16)

        @pl.when(block == 0)
        def _():
            for copy in second:
                copy.wait()
            for copy in third:
                copy.start()

        ps[...] = dot(hs[...], du[:, pl.ds(0, s.d)])
        rows = pl.ds(pl.multiple_of(block * small, small), small)
        dh_t[:, rows] = dh[rows, :].T
        norm(jnp.minimum(block + 1, blocks - 1))
        return carry

    norm(0)
    for copy in first[1:]:
        copy.wait()
    lax.fori_loop(0, blocks, forward, 0)
    for copy in third:
        copy.wait()

    quarter = s.tokens // 4

    def inner(layer, unit, block):
        cols = pl.ds(pl.multiple_of(unit * TILE, TILE), TILE)
        for half in range(quarter // TILE):
            at = block * quarter + half * TILE
            rows = pl.ds(at, TILE)
            gs[half] = dot(a[layer, rows, :], wg[:, cols])
            us[half] = dot(a[layer, rows, :], wu[:, cols])
            ds[half] = dot_t(dh[rows, :], wd[cols, :]).astype(BF16)
            for r in range(0, TILE, 32):
                part = pl.ds(r, 32)
                g, u, by = gs[half, part, :], us[half, part, :], ds[half, part, :].astype(F32)
                sig = jax.nn.sigmoid(g)
                silu = g * sig
                rows = pl.ds(at + r, 32)
                hid[rows, :] = (silu * u).astype(BF16)
                du[rows, cols] = (by * silu).astype(BF16)
                dg[rows, cols] = (by * u * (sig + silu * (1.0 - sig))).astype(BF16)

    def keep_across(slot, which, value):
        for chunk in range(s.n):
            for half in range(s.halves):
                own[slot, chunk, which, pl.ds(half * s.rows, s.rows), :] = value[
                    chunk * s.rows : (chunk + 1) * s.rows, half * LANES : (half + 1) * LANES
                ]

    def by_gate(unit, slot):
        cols = pl.ds(pl.multiple_of(unit * TILE, TILE), TILE)
        keep_across(slot, 0, dot(a_t[...], dg[:, cols]).astype(BF16))

    def by_up(unit, slot):
        cols = pl.ds(pl.multiple_of(unit * TILE, TILE), TILE)
        keep_across(slot, 1, dot(a_t[...], du[:, cols]).astype(BF16))

    def by_down(slot):
        value = dot(dh_t[...], hid[...]).T.astype(BF16)
        for which in range(2):
            for chunk in range(s.n):
                top = (which * s.n + chunk) * s.down
                for fifth in range(s.fifths):
                    own[slot, chunk, which, pl.ds(s.halves * s.rows + fifth * s.down, s.down), :] = value[
                        top : top + s.down, fifth * LANES : (fifth + 1) * LANES
                    ]

    def back_through_norm(block):
        at = block * TILE
        rows = pl.ds(pl.multiple_of(at, TILE), TILE)
        first_in[...] = dot_t(wg[...], dg[rows, :]).astype(BF16).T
        second_in[...] = dot_t(wu[...], du[rows, :]).astype(BF16).T
        for r in range(0, TILE, 32):
            part, here = pl.ds(r, 32), pl.ds(at + r, 32)
            by_a = (first_in[part, :].astype(F32) + second_in[part, :].astype(F32)).astype(BF16).astype(F32)
            wide = xh[here, :].astype(F32)
            scale = scale_of(wide)
            by = scale * by_a - wide * (scale * scale * scale * jnp.mean(wide * by_a, -1, keepdims=True))
            dh[here, :] = (dh[here, :].astype(F32) + by.astype(BF16).astype(F32)).astype(BF16)
        dh_t[:, rows] = dh[rows, :].T
        a_t[:, rows] = a[0, rows, :].T

    late = s.units + GAP

    def is_unit(u):
        return ((u >= 0) & (u < s.units)) | ((u >= late) & (u < late + s.units))

    def chunk_of(arm, hop):
        return lax.rem(me + (s.far - hop if arm == 0 else s.n - s.far + hop), s.n)

    def send(u, hop, arm, first=False):
        slot = lax.rem(u, SLOTS)
        source, target = own.at[slot, chunk_of(arm, hop)], got.at[slot, arm, hop]
        return pltpu.make_async_remote_copy(
            src_ref=source.at[arm] if first else source,
            dst_ref=target.at[arm] if first else target,
            send_sem=send_sem.at[slot, arm],
            recv_sem=recv_sem.at[slot, arm, hop],
            device_id={"dp": towards[arm]},
            device_id_type=pl.DeviceIdType.MESH,
        )

    def begin(u):
        @pl.when(is_unit(u))
        def _():
            for arm in range(2):
                send(u, 0, arm, first=True).start()

    def join(u, number, first=False):
        slot = lax.rem(u, SLOTS)
        for arm in range(2):
            before, chunk = send(u, number - 1, arm, first), chunk_of(arm, number)
            before.wait_recv()
            for half in [arm] if first else range(2):
                mine = own[slot, chunk, half].astype(F32)
                own[slot, chunk, half] = (mine + got[slot, arm, number - 1, half].astype(F32)).astype(BF16)
            before.wait_send()
        for arm in range(2):
            send(u, number, arm).start()

    def end(u):
        @pl.when(is_unit(u))
        def _():
            slot = lax.rem(u, SLOTS)
            unit = lax.select(u < late, u, u - late + s.units)
            for arm in range(2):
                before = send(u, s.far - 1, arm)
                before.wait_recv()
                before.wait_send()
            for half in range(2):
                total = own[slot, me, half].astype(F32)
                for arm in range(2):
                    total += got[slot, arm, s.far - 1, half].astype(F32)
                final[lax.div(unit, s.part), half, lax.rem(unit, s.part)] = total.astype(BF16)

    def spread(u, number, begins=False, ends=False):
        @pl.when((u >= 0) & (u < s.part))
        def _():
            for way in range(2):
                def copy(hop, source):
                    return pltpu.make_async_remote_copy(
                        src_ref=source,
                        dst_ref=gathered.at[way, hop, u],
                        send_sem=gather_send.at[u, way],
                        recv_sem=gather_recv.at[u, hop, way],
                        device_id={"dp": towards[way]},
                        device_id_type=pl.DeviceIdType.MESH,
                    )

                if not begins:
                    before = copy(number - 1, gathered.at[way, number - 1, u])
                    before.wait_recv()
                    before.wait_send()
                if not ends:
                    copy(number, final.at[0, way, u] if begins else gathered.at[way, number - 1, u]).start()

    def from_start(q):
        unit = -1
        for i, start in enumerate(GATHER_FROM):
            unit = lax.select(q == start, i, unit)
        return unit

    finish(blocks - 1, True)
    inner(1, 0, 0)
    pl.semaphore_wait(barrier, 2)

    def period(q, carry):
        early = q < s.units
        real = is_unit(q)
        layer = lax.select(early, 1, 0)
        unit = lax.select(early, q, q - late)
        slot = lax.rem(q, SLOTS)
        between = (q >= s.units) & (q < late)

        def quarter_of(k, carry):
            @pl.when(real)
            def _():
                for piece in range(2):
                    @pl.when((q == late + piece) & (k == 0))
                    def _():
                        for copy in pieces(piece):
                            copy.wait()
                inner(layer, unit, k)

            @pl.when(between)
            def _():
                back_through_norm((q - s.units) * 4 + k)

            @pl.when((k == 3) & is_unit(q - 1))
            def _():
                join(q - 1, 1, first=True)

            number = 3 - lax.div(k, 2)
            @pl.when(((k == 0) | (k == 2)) & is_unit(q - number))
            def _():
                join(q - number, number)

            back, number = lax.select(k == 3, 1, k + 2), lax.select(k == 3, 1, 2 * k + 2)
            spread(from_start(q - back), number)
            return carry

        lax.fori_loop(jnp.where(q == 0, 1, 0), 4, quarter_of, 0)

        @pl.when(q == late - 1)
        def _():
            for copy in pieces(0) + pieces(1):
                copy.start()

        @pl.when(q == late + s.units)
        def _():
            for copy in outs(0):
                copy.start()

        @pl.when(real)
        def _():
            by_gate(unit, slot)

        end(q - 3)
        spread(from_start(q - 2), 3)

        @pl.when(real)
        def _():
            by_up(unit, slot)

        spread(from_start(q - 3), 5)

        @pl.when(real)
        def _():
            by_down(slot)

        begin(q)
        spread(from_start(q - 4), s.n - 1, ends=True)
        spread(from_start(q), 0, begins=True)
        return carry

    def outs(last):
        pairs, before = [], s.part - 1
        for way in range(2):
            if last:
                pairs += [
                    (gathered.at[way, :, before], all_x[way].at[pl.ds(1, s.n - 1), before]),
                    (final.at[3, way], near_y[way].at[0]),
                ]
            else:
                pairs += [
                    (final.at[0, way], all_x[way].at[0]),
                    (gathered.at[way, :, pl.ds(0, before)], all_x[way].at[pl.ds(1, s.n - 1), pl.ds(0, before)]),
                    (final.at[1, way], near_y[way].at[1]),
                    (final.at[2, way], near_x[way]),
                ]
        return [pltpu.make_async_copy(*pair, out_sem.at[last, i]) for i, pair in enumerate(pairs)]

    def pieces(which):
        cols = pl.ds(0, TILE) if which == 0 else pl.ds(TILE, s.ff - TILE)
        return [
            pltpu.make_async_copy(wg_hbm.at[0, :, cols], wg.at[:, cols], w_sem.at[0, which]),
            pltpu.make_async_copy(wu_hbm.at[0, :, cols], wu.at[:, cols], w_sem.at[1, which]),
            pltpu.make_async_copy(wd_hbm.at[0, cols, :], wd.at[cols, :], w_sem.at[2, which]),
        ]

    lax.fori_loop(0, max(late + s.units + 2, GATHER_FROM[-1] + 4) + 1, period, 0)
    for copy in outs(1):
        copy.start()
    for copy in outs(0) + outs(1):
        copy.wait()


def reduced_shards(s, x, dy, w_gate, w_up, w_down):
    part = (s.part, s.message, LANES)
    shapes = [jax.ShapeDtypeStruct(lead + part, BF16) for lead in ((), (s.layers,), (s.n,)) for _ in range(2)]
    d, t, ff = s.d, s.tokens, s.ff
    any_space = pl.BlockSpec(memory_space=pl.ANY)
    out = pl.pallas_call(
        functools.partial(step_kernel, s),
        out_shape=shapes,
        in_specs=[any_space] * 5,
        out_specs=[any_space] * 6,
        scratch_shapes=[
            pltpu.VMEM((d, ff), BF16),
            pltpu.VMEM((d, ff), BF16),
            pltpu.VMEM((ff, d), BF16),
            pltpu.VMEM((t, d), BF16),
            pltpu.VMEM((2, t, d), BF16),
            pltpu.VMEM((d, t), BF16),
            pltpu.VMEM((t, d), BF16),
            pltpu.VMEM((d, t), BF16),
            pltpu.VMEM((t, ff), BF16),
            pltpu.VMEM((t, ff), BF16),
            pltpu.VMEM((t, TILE), BF16),
            pltpu.VMEM((SLOTS, s.n, 2, s.message, LANES), BF16),
            pltpu.VMEM((SLOTS, 2, s.far, 2, s.message, LANES), BF16),
            pltpu.VMEM((2 * s.layers, 2, *part), BF16),
            pltpu.VMEM((2, s.n - 1, *part), BF16),
            pltpu.VMEM((2, TILE, TILE), F32),
            pltpu.VMEM((2, TILE, TILE), F32),
            pltpu.VMEM((2, TILE, TILE), BF16),
            pltpu.VMEM((TILE, ff), BF16),
            pltpu.VMEM((TILE, d), F32),
            pltpu.VMEM((TILE, d), BF16),
            pltpu.VMEM((TILE, d), BF16),
            pltpu.SemaphoreType.DMA((9,)),
            pltpu.SemaphoreType.DMA((3, 2)),
            pltpu.SemaphoreType.DMA((SLOTS, 2)),
            pltpu.SemaphoreType.DMA((SLOTS, 2, s.far)),
            pltpu.SemaphoreType.DMA((2, 8)),
            pltpu.SemaphoreType.DMA((s.part, 2)),
            pltpu.SemaphoreType.DMA((s.part, s.n - 1, 2)),
        ],
        compiler_params=pltpu.CompilerParams(collective_id=0, has_side_effects=True, vmem_limit_bytes=67043328),
    )(x, dy, w_gate, w_up, w_down)
    return out[0:2], out[2:4], out[4:6]


def adamw(w, m, v, g):
    m = 0.9 * m + 0.1 * g
    v = 0.95 * v + 0.05 * g * g
    step = m * lax.rsqrt(v + 1e-8) + 0.1 * w
    return (w - 0.02 * step).astype(BF16), m, v


AHEAD = 2


def adamw_kernel(s, items, operands, *refs):
    messages, refs = refs[: 2 * operands], refs[2 * operands :]
    state, refs = (refs[0:3], refs[3:6], refs[6:9]), refs[9:]
    refs = refs[len(refs) - 24 :]
    outs, refs = (refs[0:3], refs[3:6], refs[6:9]), refs[9:]
    (message_in, across_in, down_in, across_out, down_out), (sem_in, sem_out) = (refs[0], refs[1:4], refs[4:7], refs[7:10], refs[10:13]), refs[13:15]
    me = lax.axis_index("dp")

    def of(field, item):
        values = [one[field] for one in items]
        if isinstance(item, int):
            return values[item]
        if len(set(values)) == 1:
            return values[0]
        out = values[-1]
        for i in reversed(range(len(values) - 1)):
            out = jnp.where(item == i, values[i], out)
        return out

    def places(item, way, group):
        layer, part, away = of(0, item), of(1, item), of(2, item)
        chunk = lax.rem(me + (s.n - away if way == 0 else away), s.n)
        rows = pl.ds(pl.multiple_of(chunk * s.rows, s.rows), s.rows)
        cols = pl.ds(pl.multiple_of(part * (s.part * TILE), s.part * TILE), s.part * TILE)
        units = pl.ds(part * s.part, s.part)
        return [ref.at[layer, rows, cols] for ref in group[way]] + [ref.at[layer, units, way, chunk] for ref in group[2]]

    def loads(item, way):
        spots = [ref.at[item, way] for ref in (*across_in, *down_in)]
        return [
            pltpu.make_async_copy(*pair, sem_in.at[item, way, 1 + i])
            for i, pair in enumerate(zip(places(item, way, state), spots, strict=True))
        ]

    def message_load(item, way, which):
        return pltpu.make_async_copy(messages[2 * which + way].at[of(4, item)], message_in.at[item, way], sem_in.at[item, way, 0])

    def stores(item, way):
        spots = [ref.at[item, way] for ref in (*across_out, *down_out)]
        return [
            pltpu.make_async_copy(*pair, sem_out.at[item, way, i])
            for i, pair in enumerate(zip(spots, places(item, way, outs), strict=True))
        ]

    def fetch(item, carry=0):
        for way in range(2):
            for which in range(operands):
                @pl.when(of(3, item) == which)
                def _():
                    message_load(item, way, which).start()
            for copy in loads(item, way):
                copy.start()
        return carry

    def work(item, carry):
        @pl.when(item + AHEAD < len(items))
        def _():
            fetch(item + AHEAD)

        for way in range(2):
            message_load(item, way, 0).wait()
            for copy in loads(item, way):
                copy.wait()

            def unit_step(unit, carry):
                for half in range(s.halves):
                    g = message_in[item, way, unit, pl.ds(half * s.rows, s.rows), :].astype(F32)
                    cols = pl.ds(pl.multiple_of(unit * TILE + half * LANES, LANES), LANES)
                    w, m, v = (ref[item, way, :, cols] for ref in across_in)
                    new = adamw(w.astype(F32), m, v, g)
                    for ref, value in zip(across_out, new, strict=True):
                        ref[item, way, :, cols] = value
                for fifth in range(s.fifths):
                    g = message_in[item, way, unit, pl.ds(s.halves * s.rows + fifth * s.down, s.down), :].astype(F32)
                    cols = pl.ds(fifth * LANES, LANES)
                    w, m, v = (ref[item, way, unit, :, cols] for ref in down_in)
                    new = adamw(w.astype(F32), m, v, g)
                    for ref, value in zip(down_out, new, strict=True):
                        ref[item, way, unit, :, cols] = value
                return carry

            lax.fori_loop(0, s.part, unit_step, 0)
            for copy in stores(item, way):
                copy.start()
        return carry

    def drain(item, carry):
        for way in range(2):
            for copy in stores(item, way):
                copy.wait()
        return carry

    for item in range(min(AHEAD, len(items))):
        fetch(item)
    lax.fori_loop(0, len(items), work, 0)
    lax.fori_loop(0, len(items), drain, 0)


def adamw_on(s, items, messages, state, so_far):
    flat = [one for group in state for one in group]
    shapes = [jax.ShapeDtypeStruct(one.shape, one.dtype) for one in flat]
    args = [one for pair in messages for one in pair] + flat
    aliases = {}
    if so_far is not None:
        aliases = {len(args) + i: i for i in range(9)}
        args += so_far
    count = (len(items), 2)
    across, down = (*count, s.rows, s.part * TILE), (*count, s.part, s.down, s.d)
    types = (BF16, F32, F32)
    buffers = [pltpu.VMEM(shape, dtype) for shape in (across, down) for dtype in types]
    numbers = 2 * len(items) * s.part * s.message * LANES
    any_space = pl.BlockSpec(memory_space=pl.ANY)
    return list(
        pl.pallas_call(
            functools.partial(adamw_kernel, s, items, len(messages)),
            out_shape=shapes,
            in_specs=[any_space] * len(args),
            out_specs=[any_space] * 9,
            input_output_aliases=aliases,
            scratch_shapes=[pltpu.VMEM((*count, s.part, s.message, LANES), BF16)]
            + buffers
            + buffers
            + [pltpu.SemaphoreType.DMA((*count, 7)), pltpu.SemaphoreType.DMA((*count, 6))],
            compiler_params=pltpu.CompilerParams(vmem_limit_bytes=67043328),
            cost_estimate=pl.CostEstimate(flops=numbers * 20 * 1000, bytes_accessed=numbers * 22, transcendentals=numbers),
        )(*args)
    )


def solution(mesh):
    n = mesh.shape["dp"]

    def step(x, dy, *arrays):
        weights, m, v = (arrays[i : i + 3] for i in (0, 3, 6))
        s = Sizes(mesh, x, weights[0])
        near_x, near_y, all_x = reduced_shards(s, x, dy, *weights)
        near_x = [one[None] for one in near_x]
        by_chunk = (s.layers, s.units, 2, s.n, s.down, s.d)
        state = [list(group) for group in zip(weights, m, v, strict=True)]
        state[2] = [one.reshape(by_chunk) for one in state[2]]
        rings = ([(i, (i + 1) % n) for i in range(n)], [(i, (i - 1) % n) for i in range(n)])

        def shift(pair):
            return [lax.ppermute(one, "dp", ring) for one, ring in zip(pair, rings, strict=True)]

        out, now_x, now_y = None, near_x, near_y
        for hop in range(n):
            this_x, this_y = now_x, now_y
            y_items = [(0, 1, hop, 1, 0), (1, 1, hop, 1, 1)]
            if hop < n - 1:
                if hop > 0:
                    this_y, _ = lax.optimization_barrier((this_y, before))
                    this_x, _ = lax.optimization_barrier((this_x, this_y))
                before = this_x
                now_y, now_x = shift(this_y), shift(this_x)
            here = [(1, 0, away, 0, away) for away in (range(3) if hop == 0 else [hop + 2] if hop + 2 < n else [])]
            if here:
                out = adamw_on(s, [*here, *y_items, (0, 0, hop, 2, 0)], [all_x, this_y, this_x], state, out)
            else:
                y_items = [(layer, part, away, 0, place) for layer, part, away, _, place in y_items]
                out = adamw_on(s, y_items, [this_y], state, out)
                out = adamw_on(s, [(0, 0, hop, 0, 0)], [this_x], state, out)
        out[6:9] = [one.reshape(weights[2].shape) for one in out[6:9]]
        return tuple(out[3 * which + i] for i in range(3) for which in range(3))

    return jax.shard_map(
        step,
        mesh=mesh,
        in_specs=(P(("rep", "dp"), None, None),) * 2 + (P(None, None, None),) * 9,
        out_specs=(P("rep", None, None),) * 9,
        check_vma=False,
    )
```

```python
import functools

import jax
import jax.numpy as jnp
from jax import lax
from jax.experimental import pallas as pl
from jax.experimental.pallas import tpu as pltpu
from jax.sharding import PartitionSpec as P

F32, BF16 = jnp.float32, jnp.bfloat16
LANES = 128
TILE = 256
SLOTS = 4
GAP = 2
GATHER_FROM = (6, 7, 8, 16)


def dot(a, b):
    return jnp.dot(a, b, preferred_element_type=F32)


def dot_t(a, b):
    return lax.dot_general(a, b, (((1,), (1,)), ((), ())), preferred_element_type=F32)


def scale_of(wide):
    return lax.rsqrt(jnp.mean(wide * wide, -1, keepdims=True) + 1e-6)


FLAGS = set()


class Sizes:
    def __init__(self, mesh, x, w_gate):
        self.n = mesh.shape["dp"]
        self.tokens, self.d = x.shape[1:]
        self.layers, _, self.ff = w_gate.shape
        self.units = self.ff // TILE
        self.part = self.units // 2
        self.far = self.n // 2
        self.rows = self.d // self.n
        self.down = TILE // 2 // self.n
        self.halves, self.fifths = TILE // LANES, self.d // LANES
        self.message = self.halves * self.rows + self.fifths * self.down


def step_kernel(s, x_hbm, dy_hbm, wg_hbm, wu_hbm, wd_hbm, *refs):
    (near_x, near_y, all_x), refs = (refs[0:2], refs[2:4], refs[4:6]), refs[6:]
    (wg, wu, wd, xh, a, a_t, dh, dh_t, dg, du, hid, own, got, final, gathered, gs, us, ds, hs, ps, first_in, second_in) = refs[:22]
    (load_sem, w_sem, send_sem, recv_sem), out_sems, (gather_send, gather_recv) = refs[22:26], refs[26:28], refs[28:]
    me = lax.axis_index("dp")
    right, left = lax.rem(me + 1, s.n), lax.rem(me + s.n - 1, s.n)
    towards = (right, left)

    barrier = pltpu.get_barrier_semaphore()
    for neighbour in towards:
        pl.semaphore_signal(barrier, inc=1, device_id={"dp": neighbour}, device_id_type=pl.DeviceIdType.MESH)

    small = TILE
    first = [
        pltpu.make_async_copy(x_hbm.at[0, pl.ds(0, small)], xh.at[pl.ds(0, small)], load_sem.at[0]),
        pltpu.make_async_copy(wg_hbm.at[0], dg.at[pl.ds(0, s.d)], load_sem.at[1]),
        pltpu.make_async_copy(wu_hbm.at[0], dg.at[pl.ds(s.d, s.d)], load_sem.at[2]),
    ]
    rest = s.tokens - small
    second = [
        pltpu.make_async_copy(wd_hbm.at[0], du.at[:, pl.ds(0, s.d)], load_sem.at[3]),
        pltpu.make_async_copy(dy_hbm.at[0], dh, load_sem.at[4]),
        pltpu.make_async_copy(x_hbm.at[0, pl.ds(small, rest)], xh.at[pl.ds(small, rest)], load_sem.at[8]),
    ]
    third = [
        pltpu.make_async_copy(wg_hbm.at[1], wg, load_sem.at[5]),
        pltpu.make_async_copy(wu_hbm.at[1], wu, load_sem.at[6]),
        pltpu.make_async_copy(wd_hbm.at[1], wd, load_sem.at[7]),
    ]
    for copy in first + second:
        copy.start()
    first[0].wait()

    blocks = s.tokens // small

    def norm(block):
        for r in range(0, small, 32):
            part = pl.ds(block * small + r, 32)
            wide = xh[part, :].astype(F32)
            normed = (wide * scale_of(wide)).astype(BF16)
            a[0, part, :] = normed
            first_in[pl.ds(r, 32), :] = normed

    def finish(block, ready):
        for r in range(0, small, 32):
            part = pl.ds(block * small + r, 32)
            wide = xh[part, :].astype(F32)
            h = (wide + ps[pl.ds(r, 32), :].astype(BF16).astype(F32)).astype(BF16).astype(F32)
            h = jnp.where(ready, h, wide)
            xh[part, :] = h.astype(BF16)
            normed = (h * scale_of(h)).astype(BF16)
            a[1, part, :] = normed
            second_in[pl.ds(r, 32), :] = normed
        a_t[:, pl.ds(pl.multiple_of(block * small, small), small)] = second_in[...].T

    def forward(block, carry):
        finish(jnp.maximum(block - 1, 0), block > 0)
        for j in range(s.units):
            cols = pl.ds(j * TILE, TILE)
            gs[j % 2] = dot(first_in[...], dg[pl.ds(0, s.d), cols])
            us[j % 2] = dot(first_in[...], dg[pl.ds(s.d, s.d), cols])
            for r in range(0, small, 32):
                g = gs[j % 2, pl.ds(r, 32), :]
                hs[pl.ds(r, 32), cols] = (g * jax.nn.sigmoid(g) * us[j % 2, pl.ds(r, 32), :]).astype(BF16)

        @pl.when(block == 0)
        def _():
            for copy in second:
                copy.wait()
            for copy in third:
                copy.start()

        ps[...] = dot(hs[...], du[:, pl.ds(0, s.d)])
        rows = pl.ds(pl.multiple_of(block * small, small), small)
        dh_t[:, rows] = dh[rows, :].T
        norm(jnp.minimum(block + 1, blocks - 1))
        return carry

    norm(0)
    for copy in first[1:]:
        copy.wait()
    lax.fori_loop(0, blocks, forward, 0)
    for copy in third:
        copy.wait()

    quarter = s.tokens // 4

    def inner(layer, unit, block):
        cols = pl.ds(pl.multiple_of(unit * TILE, TILE), TILE)
        for half in range(quarter // TILE):
            at = block * quarter + half * TILE
            rows = pl.ds(at, TILE)
            gs[half] = dot(a[layer, rows, :], wg[:, cols])
            us[half] = dot(a[layer, rows, :], wu[:, cols])
            ds[half] = dot_t(dh[rows, :], wd[cols, :]).astype(BF16)
            for r in range(0, TILE, 32):
                part = pl.ds(r, 32)
                g, u, by = gs[half, part, :], us[half, part, :], ds[half, part, :].astype(F32)
                sig = jax.nn.sigmoid(g)
                silu = g * sig
                rows = pl.ds(at + r, 32)
                hid[rows, :] = (silu * u).astype(BF16)
                du[rows, cols] = (by * silu).astype(BF16)
                dg[rows, cols] = (by * u * (sig + silu * (1.0 - sig))).astype(BF16)

    def keep_across(slot, which, value):
        for chunk in range(s.n):
            for half in range(s.halves):
                own[slot, chunk, which, pl.ds(half * s.rows, s.rows), :] = value[
                    chunk * s.rows : (chunk + 1) * s.rows, half * LANES : (half + 1) * LANES
                ]

    def by_gate(unit, slot):
        cols = pl.ds(pl.multiple_of(unit * TILE, TILE), TILE)
        keep_across(slot, 0, dot(a_t[...], dg[:, cols]).astype(BF16))

    def by_up(unit, slot):
        cols = pl.ds(pl.multiple_of(unit * TILE, TILE), TILE)
        keep_across(slot, 1, dot(a_t[...], du[:, cols]).astype(BF16))

    def by_down(slot):
        value = dot(dh_t[...], hid[...]).T.astype(BF16)
        for which in range(2):
            for chunk in range(s.n):
                top = (which * s.n + chunk) * s.down
                for fifth in range(s.fifths):
                    own[slot, chunk, which, pl.ds(s.halves * s.rows + fifth * s.down, s.down), :] = value[
                        top : top + s.down, fifth * LANES : (fifth + 1) * LANES
                    ]

    def back_through_norm(block):
        at = block * TILE
        rows = pl.ds(pl.multiple_of(at, TILE), TILE)
        first_in[...] = dot_t(wg[...], dg[rows, :]).astype(BF16).T
        second_in[...] = dot_t(wu[...], du[rows, :]).astype(BF16).T
        for r in range(0, TILE, 32):
            part, here = pl.ds(r, 32), pl.ds(at + r, 32)
            by_a = (first_in[part, :].astype(F32) + second_in[part, :].astype(F32)).astype(BF16).astype(F32)
            wide = xh[here, :].astype(F32)
            scale = scale_of(wide)
            by = scale * by_a - wide * (scale * scale * scale * jnp.mean(wide * by_a, -1, keepdims=True))
            dh[here, :] = (dh[here, :].astype(F32) + by.astype(BF16).astype(F32)).astype(BF16)
        dh_t[:, rows] = dh[rows, :].T
        a_t[:, rows] = a[0, rows, :].T

    late = s.units + GAP

    def is_unit(u):
        return ((u >= 0) & (u < s.units)) | ((u >= late) & (u < late + s.units))

    def chunk_of(arm, hop):
        return lax.rem(me + (s.far - hop if arm == 0 else s.n - s.far + hop), s.n)

    def send(u, hop, arm, first=False):
        slot = lax.rem(u, SLOTS)
        source, target = own.at[slot, chunk_of(arm, hop)], got.at[slot, arm, hop]
        return pltpu.make_async_remote_copy(
            src_ref=source.at[arm] if first else source,
            dst_ref=target.at[arm] if first else target,
            send_sem=send_sem.at[slot, arm],
            recv_sem=recv_sem.at[slot, arm, hop],
            device_id={"dp": towards[arm]},
            device_id_type=pl.DeviceIdType.MESH,
        )

    def begin(u):
        @pl.when(is_unit(u))
        def _():
            for arm in range(2):
                send(u, 0, arm, first=True).start()

    def join(u, number, first=False):
        slot = lax.rem(u, SLOTS)
        for arm in range(2):
            before, chunk = send(u, number - 1, arm, first), chunk_of(arm, number)
            before.wait_recv()
            for half in [arm] if first else range(2):
                mine = own[slot, chunk, half].astype(F32)
                own[slot, chunk, half] = (mine + got[slot, arm, number - 1, half].astype(F32)).astype(BF16)
            before.wait_send()
        for arm in range(2):
            send(u, number, arm).start()

    def end(u):
        @pl.when(is_unit(u))
        def _():
            slot = lax.rem(u, SLOTS)
            unit = lax.select(u < late, u, u - late + s.units)
            for arm in range(2):
                before = send(u, s.far - 1, arm)
                before.wait_recv()
                before.wait_send()
            for half in range(2):
                total = own[slot, me, half].astype(F32)
                for arm in range(2):
                    total += got[slot, arm, s.far - 1, half].astype(F32)
                final[lax.div(unit, s.part), half, lax.rem(unit, s.part)] = total.astype(BF16)

    def spread(u, number, begins=False, ends=False):
        @pl.when((u >= 0) & (u < s.part))
        def _():
            for way in range(2):
                def copy(hop, source):
                    return pltpu.make_async_remote_copy(
                        src_ref=source,
                        dst_ref=gathered.at[way, hop, u],
                        send_sem=gather_send.at[u, way],
                        recv_sem=gather_recv.at[u, hop, way],
                        device_id={"dp": towards[way]},
                        device_id_type=pl.DeviceIdType.MESH,
                    )

                if not begins:
                    before = copy(number - 1, gathered.at[way, number - 1, u])
                    before.wait_recv()
                    before.wait_send()
                if not ends:
                    copy(number, final.at[0, way, u] if begins else gathered.at[way, number - 1, u]).start()

    def from_start(q):
        unit = -1
        for i, start in enumerate(GATHER_FROM):
            unit = lax.select(q == start, i, unit)
        return unit

    inner(1, 0, 0)
    finish(blocks - 1, True)
    pl.semaphore_wait(barrier, 2)

    def period(q, carry):
        early = q < s.units
        real = is_unit(q)
        layer = lax.select(early, 1, 0)
        unit = lax.select(early, q, q - late)
        slot = lax.rem(q, SLOTS)
        between = (q >= s.units) & (q < late)

        def quarter_of(k, carry):
            @pl.when(real)
            def _():
                for piece in range(2):
                    @pl.when((q == late + piece) & (k == 0))
                    def _():
                        for copy in pieces(piece):
                            copy.wait()
                inner(layer, unit, k)

            @pl.when(between)
            def _():
                back_through_norm((q - s.units) * 4 + k)

            @pl.when((k == 3) & is_unit(q - 1))
            def _():
                join(q - 1, 1, first=True)

            number = 3 - lax.div(k, 2)
            @pl.when(((k == 0) | (k == 2)) & is_unit(q - number))
            def _():
                join(q - number, number)

            back, number = lax.select(k == 3, 1, k + 2), lax.select(k == 3, 1, 2 * k + 2)
            spread(from_start(q - back), number)
            return carry

        lax.fori_loop(jnp.where(q == 0, 1, 0), 4, quarter_of, 0)

        @pl.when(q == late - 1)
        def _():
            for copy in pieces(0) + pieces(1):
                copy.start()

        @pl.when(q == late + s.units + 2)
        def _():
            for copy in outs(0):
                copy.start()

        @pl.when(real)
        def _():
            by_gate(unit, slot)

        end(q - 3)
        spread(from_start(q - 2), 3)

        @pl.when(real)
        def _():
            by_up(unit, slot)

        spread(from_start(q - 3), 5)

        @pl.when(real)
        def _():
            by_down(slot)

        begin(q)
        spread(from_start(q - 4), s.n - 1, ends=True)
        spread(from_start(q), 0, begins=True)
        return carry

    def outs(last):
        pairs, before = [], s.part - 1
        for way in range(2):
            x, y, half = near_x[way], near_y[way], s.part // 2
            if last:
                pairs += [
                    (gathered.at[way, :, before], all_x[way].at[pl.ds(1, s.n - 1), before]),
                    (final.at[3, way, pl.ds(before, 1)], y.at[pl.ds(before, 1)]),
                ]
            else:
                pairs += [
                    (final.at[0, way], all_x[way].at[0]),
                    (gathered.at[way, :, pl.ds(0, before)], all_x[way].at[pl.ds(1, s.n - 1), pl.ds(0, before)]),
                    (final.at[2, way], x.at[pl.ds(0, s.part)]),
                    (final.at[1, way, pl.ds(0, half)], x.at[pl.ds(s.part, half)]),
                    (final.at[1, way, pl.ds(half, half)], y.at[pl.ds(s.part, half)]),
                    (final.at[3, way, pl.ds(0, before)], y.at[pl.ds(0, before)]),
                ]
        return [pltpu.make_async_copy(*pair, out_sems[last].at[i]) for i, pair in enumerate(pairs)]

    def pieces(which):
        cols = pl.ds(0, TILE) if which == 0 else pl.ds(TILE, s.ff - TILE)
        return [
            pltpu.make_async_copy(wg_hbm.at[0, :, cols], wg.at[:, cols], w_sem.at[0, which]),
            pltpu.make_async_copy(wu_hbm.at[0, :, cols], wu.at[:, cols], w_sem.at[1, which]),
            pltpu.make_async_copy(wd_hbm.at[0, cols, :], wd.at[cols, :], w_sem.at[2, which]),
        ]

    lax.fori_loop(0, max(late + s.units + 2, GATHER_FROM[-1] + 4) + 1, period, 0)
    for copy in outs(1):
        copy.start()
    for copy in outs(0) + outs(1):
        copy.wait()


def reduced_shards(s, x, dy, w_gate, w_up, w_down):
    part = (s.part, s.message, LANES)
    ring = (s.part + s.part // 2, s.message, LANES)
    shapes = [jax.ShapeDtypeStruct(shape, BF16) for shape in (ring, ring, (s.n, *part)) for _ in range(2)]
    d, t, ff = s.d, s.tokens, s.ff
    any_space = pl.BlockSpec(memory_space=pl.ANY)
    out = pl.pallas_call(
        functools.partial(step_kernel, s),
        out_shape=shapes,
        in_specs=[any_space] * 5,
        out_specs=[any_space] * 6,
        scratch_shapes=[
            pltpu.VMEM((d, ff), BF16),
            pltpu.VMEM((d, ff), BF16),
            pltpu.VMEM((ff, d), BF16),
            pltpu.VMEM((t, d), BF16),
            pltpu.VMEM((2, t, d), BF16),
            pltpu.VMEM((d, t), BF16),
            pltpu.VMEM((t, d), BF16),
            pltpu.VMEM((d, t), BF16),
            pltpu.VMEM((t, ff), BF16),
            pltpu.VMEM((t, ff), BF16),
            pltpu.VMEM((t, TILE), BF16),
            pltpu.VMEM((SLOTS, s.n, 2, s.message, LANES), BF16),
            pltpu.VMEM((SLOTS, 2, s.far, 2, s.message, LANES), BF16),
            pltpu.VMEM((2 * s.layers, 2, *part), BF16),
            pltpu.VMEM((2, s.n - 1, *part), BF16),
            pltpu.VMEM((2, TILE, TILE), F32),
            pltpu.VMEM((2, TILE, TILE), F32),
            pltpu.VMEM((2, TILE, TILE), BF16),
            pltpu.VMEM((TILE, ff), BF16),
            pltpu.VMEM((TILE, d), F32),
            pltpu.VMEM((TILE, d), BF16),
            pltpu.VMEM((TILE, d), BF16),
            pltpu.SemaphoreType.DMA((9,)),
            pltpu.SemaphoreType.DMA((3, 2)),
            pltpu.SemaphoreType.DMA((SLOTS, 2)),
            pltpu.SemaphoreType.DMA((SLOTS, 2, s.far)),
            pltpu.SemaphoreType.DMA((12,)),
            pltpu.SemaphoreType.DMA((4,)),
            pltpu.SemaphoreType.DMA((s.part, 2)),
            pltpu.SemaphoreType.DMA((s.part, s.n - 1, 2)),
        ],
        compiler_params=pltpu.CompilerParams(collective_id=0, has_side_effects=True, vmem_limit_bytes=67043328),
    )(x, dy, w_gate, w_up, w_down)
    return out[0:2], out[2:4], out[4:6]


def adamw(w, m, v, g):
    m = 0.9 * m + 0.1 * g
    v = 0.95 * v + 0.05 * g * g
    step = m * lax.rsqrt(v + 1e-8) + 0.1 * w
    return (w - 0.02 * step).astype(BF16), m, v


AHEAD = 2


def adamw_kernel(s, span, items, operands, *refs):
    messages, refs = refs[: 2 * operands], refs[2 * operands :]
    state, refs = (refs[0:3], refs[3:6], refs[6:9]), refs[9:]
    refs = refs[len(refs) - 24 :]
    outs, refs = (refs[0:3], refs[3:6], refs[6:9]), refs[9:]
    (message_in, across_in, down_in, across_out, down_out), (sem_in, sem_out) = (refs[0], refs[1:4], refs[4:7], refs[7:10], refs[10:13]), refs[13:15]
    me = lax.axis_index("dp")

    def of(field, item):
        values = [one[field] for one in items]
        if isinstance(item, int):
            return values[item]
        if len(set(values)) == 1:
            return values[0]
        out = values[-1]
        for i in reversed(range(len(values) - 1)):
            out = jnp.where(item == i, values[i], out)
        return out

    def places(item, way, group):
        layer, first, away = of(0, item), of(1, item), of(2, item)
        chunk = lax.rem(me + (s.n - away if way == 0 else away), s.n)
        rows = pl.ds(pl.multiple_of(chunk * s.rows, s.rows), s.rows)
        cols = pl.ds(pl.multiple_of(first * TILE, span * TILE), span * TILE)
        units = pl.ds(first, span)
        return [ref.at[layer, rows, cols] for ref in group[way]] + [ref.at[layer, units, way, chunk] for ref in group[2]]

    def loads(item, way):
        spots = [ref.at[item, way] for ref in (*across_in, *down_in)]
        return [
            pltpu.make_async_copy(*pair, sem_in.at[lax.rem(item, AHEAD + 1), way, 2 + i])
            for i, pair in enumerate(zip(places(item, way, state), spots, strict=True))
        ]

    def message_loads(item, way, act):
        for number, one in enumerate(items):
            @pl.when(item == number)
            def _():
                at = 0
                for i, (which, start, count) in enumerate(one[3]):
                    spot = message_in.at[number, way, pl.ds(at, count)]
                    act(pltpu.make_async_copy(messages[2 * which + way].at[pl.ds(start, count)], spot, sem_in.at[number % (AHEAD + 1), way, i]))
                    at += count

    def stores(item, way):
        spots = [ref.at[item, way] for ref in (*across_out, *down_out)]
        return [
            pltpu.make_async_copy(*pair, sem_out.at[lax.rem(item, AHEAD), way, i])
            for i, pair in enumerate(zip(spots, places(item, way, outs), strict=True))
        ]

    def fetch(item, carry=0):
        for way in range(2):
            message_loads(item, way, lambda copy: copy.start())
            for copy in loads(item, way):
                copy.start()
        return carry

    def work(item, carry):
        @pl.when(item + AHEAD < len(items))
        def _():
            fetch(item + AHEAD)

        for way in range(2):
            message_loads(item, way, lambda copy: copy.wait())
            for copy in loads(item, way):
                copy.wait()

            def unit_step(unit, carry):
                for half in range(s.halves):
                    g = message_in[item, way, unit, pl.ds(half * s.rows, s.rows), :].astype(F32)
                    cols = pl.ds(pl.multiple_of(unit * TILE + half * LANES, LANES), LANES)
                    w, m, v = (ref[item, way, :, cols] for ref in across_in)
                    new = adamw(w.astype(F32), m, v, g)
                    for ref, value in zip(across_out, new, strict=True):
                        ref[item, way, :, cols] = value
                for fifth in range(s.fifths):
                    g = message_in[item, way, unit, pl.ds(s.halves * s.rows + fifth * s.down, s.down), :].astype(F32)
                    cols = pl.ds(fifth * LANES, LANES)
                    w, m, v = (ref[item, way, unit, :, cols] for ref in down_in)
                    new = adamw(w.astype(F32), m, v, g)
                    for ref, value in zip(down_out, new, strict=True):
                        ref[item, way, unit, :, cols] = value
                return carry

            lax.fori_loop(0, span, unit_step, 0)

            @pl.when(item >= AHEAD)
            def _():
                for copy in stores(item - AHEAD, way):
                    copy.wait()

            for copy in stores(item, way):
                copy.start()
        return carry

    def drain(item, carry):
        for way in range(2):
            for copy in stores(item, way):
                copy.wait()
        return carry

    for item in range(min(AHEAD, len(items))):
        fetch(jnp.int32(item))
    lax.fori_loop(0, len(items), work, 0)
    lax.fori_loop(max(len(items) - AHEAD, 0), len(items), drain, 0)


def adamw_on(s, span, items, messages, state, so_far):
    flat = [one for group in state for one in group]
    shapes = [jax.ShapeDtypeStruct(one.shape, one.dtype) for one in flat]
    args = [one for pair in messages for one in pair] + flat
    aliases = {}
    if so_far is not None:
        aliases = {len(args) + i: i for i in range(9)}
        args += so_far
    count = (len(items), 2)
    across, down = (*count, s.rows, span * TILE), (*count, span, s.down, s.d)
    types = (BF16, F32, F32)
    buffers = [pltpu.VMEM(shape, dtype) for shape in (across, down) for dtype in types]
    numbers = 2 * len(items) * span * s.message * LANES
    any_space = pl.BlockSpec(memory_space=pl.ANY)
    return list(
        pl.pallas_call(
            functools.partial(adamw_kernel, s, span, items, len(messages)),
            out_shape=shapes,
            in_specs=[any_space] * len(args),
            out_specs=[any_space] * 9,
            input_output_aliases=aliases,
            scratch_shapes=[pltpu.VMEM((*count, span, s.message, LANES), BF16)]
            + buffers
            + buffers
            + [pltpu.SemaphoreType.DMA((AHEAD + 1, 2, 8)), pltpu.SemaphoreType.DMA((AHEAD, 2, 6))],
            compiler_params=pltpu.CompilerParams(vmem_limit_bytes=67043328),
            cost_estimate=pl.CostEstimate(flops=numbers * 20 * 1000, bytes_accessed=numbers * 22, transcendentals=numbers),
        )(*args)
    )


def solution(mesh):
    n = mesh.shape["dp"]

    def step(x, dy, *arrays):
        weights, m, v = (arrays[i : i + 3] for i in (0, 3, 6))
        s = Sizes(mesh, x, weights[0])
        near_x, near_y, all_x = reduced_shards(s, x, dy, *weights)
        all_x = [one.reshape(n * s.part, s.message, LANES) for one in all_x]
        by_chunk = (s.layers, s.units, 2, s.n, s.down, s.d)
        state = [list(group) for group in zip(weights, m, v, strict=True)]
        state[2] = [one.reshape(by_chunk) for one in state[2]]
        rings = ([(i, (i + 1) % n) for i in range(n)], [(i, (i - 1) % n) for i in range(n)])

        def shift(pair):
            return [lax.ppermute(one, "dp", ring) for one, ring in zip(pair, rings, strict=True)]

        out, now_x, now_y = None, near_x, near_y
        part, half = s.part, s.part // 2
        for hop in range(n):
            this_x, this_y = now_x, now_y
            if hop < n - 1:
                if hop > 0:
                    this_y, _ = lax.optimization_barrier((this_y, before))
                    this_x, _ = lax.optimization_barrier((this_x, this_y))
                before = this_x
                now_y, now_x = shift(this_y), shift(this_x)
                early = range(2) if hop == 0 else [hop + 1]
                items = [(1, 0, away, ((2, away * part, part),)) for away in early]
                items += [(0, part, hop, ((1, 0, part),)), (1, part, hop, ((0, part, half), (1, part, half))), (0, 0, hop, ((0, 0, part),))]
                out = adamw_on(s, part, items, [this_x, this_y, all_x], state, out)
            else:
                for messages, first in ((this_y, part), (this_x, 0)):
                    items = [(0, first + i, hop, ((0, i, half),)) for i in range(0, part, half)]
                    items += [(1, part + (half if first else 0), hop, ((0, part, half),))]
                    out = adamw_on(s, half, items, [messages], state, out)
        out[6:9] = [one.reshape(weights[2].shape) for one in out[6:9]]
        return tuple(out[3 * which + i] for i in range(3) for which in range(3))

    return jax.shard_map(
        step,
        mesh=mesh,
        in_specs=(P(("rep", "dp"), None, None),) * 2 + (P(None, None, None),) * 9,
        out_specs=(P("rep", None, None),) * 9,
        check_vma=False,
    )
```
